256 devices in a mesh: seq: 64 (over y_lo, x, z), tensor: 4 (over y_hi, core).
Axes of the slice: x: 4, y: 4 (y_hi: 2, y_lo: 2; y = y_hi * 2 + y_lo), z: 8, core: 2. Of those that a mesh axis runs over, the one named last changes fastest.
Arguments:
- tokens: bfloat16 [32768, 2048], P('seq', 'tensor'), may hold values from -12 to 12
- attn_gain: float32 [2048], replicated, may hold values from 0.1 to 1.9
- w_query: bfloat16 [2048, 2048], P('seq', 'tensor'), as said below
- w_key: bfloat16 [2048, 512], P('seq', 'tensor'), as said below
- w_value: bfloat16 [2048, 512], P('seq', 'tensor'), may hold values from -0.125 to 0.125
- w_out: bfloat16 [2048, 2048], P('tensor', 'seq'), may hold values from -0.125 to 0.125
- mlp_gain: float32 [2048], replicated, may hold values from 0.1 to 1.9
- w_gate: bfloat16 [2048, 5632], P('seq', 'tensor'), may hold values from -0.125 to 0.125
- w_up: bfloat16 [2048, 5632], P('seq', 'tensor'), may hold values from -0.125 to 0.125
- w_down: bfloat16 [5632, 2048], P('tensor', 'seq'), may hold values from -0.078125 to 0.078125
Outputs:
- layer_out: bfloat16 [32768, 2048], P('seq', 'tensor')
The draws below stay inside these ranges and needn't reach their ends.
Inputs may be any that keep to these rules, and one draw needn't show every extreme that they name: `w_query`: entries are of order 2048 to the power -1/2. `w_key`: entries are of order 2048 to the power -1/2.
All inputs are finite; a program needn't handle non-finite values.
Results may differ from the reference program's by a relative error of at most 0.013.
Values may be sent and summed in bfloat16 or wider, within the bound.
No kernel may reach another device: no remote copies, remote signals or barrier semaphores. Data moves between devices by JAX's collectives and lax.ppermute only.
A program may use at most 128 MiB of HBM per device.

```python
import jax
import jax.numpy as jnp
from jax import lax

D = 2048
HEADS = 16
KV_HEADS = 4
HEAD_DIM = 128
FF = 5632
WINDOW = 1024
TOK_DEV = 512
TOKENS = 32768


def draw_tokens(key, part):
    noise = jax.random.normal(jax.random.fold_in(key, 31), (TOKENS, D), jnp.float32)
    return jnp.clip(noise, -12.0, 12.0).astype(jnp.bfloat16)


def draw_w_query(key, part):
    base = jax.random.normal(jax.random.fold_in(key, 21), (D, HEADS * HEAD_DIM), jnp.float32) / jnp.sqrt(1.0 * D)
    bound = 9.0 / jnp.sqrt(1.0 * D)
    return jnp.clip(base, -bound, bound).astype(jnp.bfloat16)


def draw_w_key(key, part):
    base = jax.random.normal(jax.random.fold_in(key, 22), (D, KV_HEADS * HEAD_DIM), jnp.float32) / jnp.sqrt(1.0 * D)
    bound = 9.0 / jnp.sqrt(1.0 * D)
    return jnp.clip(base, -bound, bound).astype(jnp.bfloat16)


def level_of(rng, extent, pieces, smallest, largest):
    level = 1.0
    for axis_at, shards_of in pieces:
        draws = jax.random.uniform(jax.random.fold_in(jax.random.fold_in(rng, 6), axis_at), (shards_of,), jnp.float32, smallest / len(pieces), largest / len(pieces))
        level = level * jnp.repeat(jnp.exp(draws), extent[axis_at] // shards_of).reshape((-1,) + (1,) * (len(extent) - 1 - axis_at))
    return level


def scatter_about(rng, shape, width, most, shards=(), kind=jnp.bfloat16):
    result = width * jax.random.normal(rng, shape, jnp.float32)
    if shards:
        result = result * level_of(rng, shape, shards, -0.22, 0.18)
    return jnp.clip(result, -most, most).astype(kind)


def setup_inputs(seed: int = 0) -> dict:
    arg_keys = jax.random.split(jax.random.key(seed), 11)
    return {
        "tokens": draw_tokens(jax.random.fold_in(arg_keys[10], 71), 0),
        "attn_gain": jnp.clip(1.0 + 0.18 * jax.random.normal(arg_keys[1], (D,), jnp.float32), 0.1, 1.9),
        "w_query": draw_w_query(jax.random.fold_in(arg_keys[10], 71), 0),
        "w_key": draw_w_key(jax.random.fold_in(arg_keys[10], 71), 0),
        "w_value": scatter_about(arg_keys[4], (D, KV_HEADS * HEAD_DIM), D ** -0.5, 0.125, ((0, 64), (1, 4))),
        "w_out": scatter_about(arg_keys[5], (HEADS * HEAD_DIM, D), (HEADS * HEAD_DIM) ** -0.5, 0.125, ((0, 4), (1, 64))),
        "mlp_gain": jnp.clip(1.0 + 0.18 * jax.random.normal(arg_keys[6], (D,), jnp.float32), 0.1, 1.9),
        "w_gate": scatter_about(arg_keys[7], (D, FF), D ** -0.5, 0.125, ((0, 64), (1, 4))),
        "w_up": scatter_about(arg_keys[8], (D, FF), D ** -0.5, 0.125, ((0, 64), (1, 4))),
        "w_down": scatter_about(arg_keys[9], (FF, D), FF ** -0.5, 0.078125, ((0, 4), (1, 64))),
    }


def scaled_rows(values, gain):
    values = values.astype(jnp.float32)
    mean_square = lax.optimization_barrier(jnp.mean(values * values, axis=1, keepdims=True))
    return (values * lax.rsqrt(mean_square + 1e-06) * gain.astype(jnp.float32)).astype(jnp.bfloat16)

def reference(tokens, attn_gain, w_query, w_key, w_value, w_out, mlp_gain, w_gate, w_up, w_down):
    normed = scaled_rows(tokens, attn_gain)
    queries = jnp.dot(normed, w_query, preferred_element_type=jnp.float32).astype(jnp.bfloat16)
    keys = jnp.dot(normed, w_key, preferred_element_type=jnp.float32).astype(jnp.bfloat16)
    values = jnp.dot(normed, w_value, preferred_element_type=jnp.float32).astype(jnp.bfloat16)
    group = HEADS // KV_HEADS
    block = min(512, TOK_DEV)
    count = TOKENS // block
    span = WINDOW + block
    scale = HEAD_DIM ** (-0.5)
    grouped = queries.reshape(TOKENS, KV_HEADS, group, HEAD_DIM)
    padding = jnp.zeros((WINDOW, KV_HEADS * HEAD_DIM), keys.dtype)
    keys_padded = jnp.concatenate([padding, keys], axis=0)
    values_padded = jnp.concatenate([padding, values], axis=0)

    def one_block(index):
        start = (index * block).astype(jnp.int32)
        query_block = lax.dynamic_slice_in_dim(grouped, start, block, 0)
        key_block = lax.dynamic_slice_in_dim(keys_padded, start, span, 0).reshape(span, KV_HEADS, HEAD_DIM)
        value_block = lax.dynamic_slice_in_dim(values_padded, start, span, 0).reshape(span, KV_HEADS, HEAD_DIM)
        scores = jnp.einsum('qkgd,ckd->kgqc', query_block.astype(jnp.float32), key_block.astype(jnp.float32)) * scale
        query_pos = lax.broadcasted_iota(jnp.int32, (block, span), 0)
        key_pos = lax.broadcasted_iota(jnp.int32, (block, span), 1)
        distance = query_pos + WINDOW - key_pos
        allowed = (distance >= 0) & (distance < WINDOW) & (key_pos + start - WINDOW >= 0)
        scores = jnp.where(allowed[None, None], scores, -1e+30)
        highest = lax.optimization_barrier(jnp.max(scores, axis=3, keepdims=True))
        raised = jnp.exp(scores - highest)
        weights = (raised / lax.optimization_barrier(jnp.sum(raised, axis=3, keepdims=True))).astype(jnp.bfloat16)
        mixed = jnp.einsum('kgqc,ckd->qkgd', weights.astype(jnp.float32), value_block.astype(jnp.float32))
        return mixed.astype(jnp.bfloat16).reshape(block, HEADS * HEAD_DIM)
    attended = lax.map(one_block, jnp.arange(count, dtype=jnp.int32)).reshape(TOKENS, HEADS * HEAD_DIM)
    group_width = group * HEAD_DIM
    attn_sum = jnp.zeros((TOKENS, D), jnp.float32)
    for head_group in range(KV_HEADS):
        lower = head_group * group_width
        term = jnp.dot(attended[:, lower:lower + group_width], w_out[lower:lower + group_width], preferred_element_type=jnp.float32)
        term = lax.optimization_barrier(term.astype(jnp.bfloat16))
        attn_sum = attn_sum + term.astype(jnp.float32)
    stream = (tokens.astype(jnp.float32) + attn_sum).astype(jnp.bfloat16)
    stream_normed = scaled_rows(stream, mlp_gain)
    gate = jnp.dot(stream_normed, w_gate, preferred_element_type=jnp.float32)
    upward = jnp.dot(stream_normed, w_up, preferred_element_type=jnp.float32)
    hidden = (jax.nn.silu(gate) * upward).astype(jnp.bfloat16)
    block_width = FF // KV_HEADS
    mlp_sum = jnp.zeros((TOKENS, D), jnp.float32)
    for unit_block in range(KV_HEADS):
        lower = unit_block * block_width
        term = jnp.dot(hidden[:, lower:lower + block_width], w_down[lower:lower + block_width], preferred_element_type=jnp.float32)
        term = lax.optimization_barrier(term.astype(jnp.bfloat16))
        mlp_sum = mlp_sum + term.astype(jnp.float32)
    return (stream.astype(jnp.float32) + mlp_sum).astype(jnp.bfloat16)
```

```python
import jax
import jax.numpy as jnp
from jax import lax
from jax.sharding import Mesh
from jax.sharding import PartitionSpec as P

HEAD_DIM = 128
WINDOW = 1024
SEQ = ("yl", "x", "z")
FEATURES = ("yh", "c")
PLANE = ("x", "z")


def spread(value, axis):
    length = lax.axis_size(axis)
    return lax.all_to_all(
        jnp.broadcast_to(value[None], (length, *value.shape)), axis, 0, 0, tiled=True
    )


def plane_rows(value):
    tiles = spread(value, "z")
    tiles = tiles.reshape(-1, value.shape[1])
    return spread(tiles, "x").reshape(-1, value.shape[1])


def other_core(value):
    return lax.ppermute(value, "c", [(0, 1), (1, 0)])


def column_partner(value, flip):
    return lax.ppermute(value, ("yl", "yh"), [(i, i ^ flip) for i in range(4)])


def ordered(flag, first, second):
    return jnp.where(flag == 0, first, second), jnp.where(flag == 0, second, first)


def shuffled_rows(parts):
    count = lax.axis_size("yl") * lax.axis_size("x") * lax.axis_size("z")
    core = lax.axis_index("c")
    parity = lax.axis_index("z") % 2
    received = []
    for swap, send in enumerate(ordered(parity, parts[0], parts[1])):
        route = []
        for block in range(count):
            for head in range(2):
                to_core = block % 2 if swap == 0 else 1 - block % 2
                target = (head * (count // 2) + block // 2) * 2 + to_core
                route.append((block * 2 + head, target))
        received.append(lax.ppermute(send, ("yl", "x", "z", "c"), route))
    return jnp.concatenate(ordered(core, received[0], received[1]), axis=0)


def column_tokens(share):
    yh, core = lax.axis_index("yh"), lax.axis_index("c")
    blocks = [share] + [column_partner(share, flip) for flip in (1, 2, 3)]
    mine = jnp.stack(blocks)
    theirs = other_core(mine)
    runs = []
    for run in range(2):
        pairs = []
        for half in range(2):
            pairs.append(ordered(core, mine[run * 2 + half], theirs[run * 2 + half]))
        features = []
        for core_at in range(2):
            features.append(ordered(yh, pairs[0][core_at], pairs[1][core_at]))
        runs.append(
            jnp.concatenate(
                [features[0][0], features[1][0], features[0][1], features[1][1]], axis=1
            )
        )
    return jnp.concatenate(runs, axis=0)


def scaled_rows(values, gain):
    values = values.astype(jnp.float32)
    mean_square = jnp.mean(values * values, axis=1, keepdims=True)
    return (values * lax.rsqrt(mean_square + 1e-06) * gain).astype(jnp.bfloat16)


def product(left, right):
    return jnp.dot(left, right, preferred_element_type=jnp.float32)


def product_t(left, right):
    return lax.dot_general(
        left, right, (((1,), (1,)), ((), ())), preferred_element_type=jnp.float32
    )


def column_sum(left, blocks):
    rows = left.shape[0] // 2
    mine = lax.axis_index("yh") * 2 + lax.axis_index("c")

    def term(flip):
        block = lax.dynamic_index_in_dim(blocks, mine ^ flip, 0, keepdims=False)
        return product_t(left, block)

    away = jnp.stack([term(1), term(3)]).astype(jnp.bfloat16)
    came = other_core(away).astype(jnp.float32)
    near = term(0) + came[0]
    far = term(2) + came[1]
    total = near[:rows]
    sent = (
        (far[:rows], 1),
        (near[rows:], 2),
        (far[rows:], 3),
    )
    for value, flip in sent:
        total = total + column_partner(value.astype(jnp.bfloat16), flip).astype(jnp.float32)
    return total


def window_attention(queries, keys, values, first_key):
    rows = queries.shape[1]
    span = keys.shape[1]
    scale = HEAD_DIM ** (-0.5)
    scores = jnp.einsum("rqhd,rcd->rhqc", queries, keys, preferred_element_type=jnp.float32) * scale
    query_pos = lax.broadcasted_iota(jnp.int32, (rows, span), 0)
    key_pos = lax.broadcasted_iota(jnp.int32, (rows, span), 1)
    distance = query_pos + WINDOW - key_pos
    inside = (distance >= 0) & (distance < WINDOW)
    allowed = inside[None] & (key_pos[None] + first_key[:, None, None] >= 0)
    scores = jnp.where(allowed[:, None], scores, -1e30)
    highest = jnp.max(scores, axis=3, keepdims=True)
    raised = jnp.exp(scores - highest)
    weights = (raised / jnp.sum(raised, axis=3, keepdims=True)).astype(jnp.bfloat16)
    mixed = jnp.einsum("rhqc,rcd->rqhd", weights, values, preferred_element_type=jnp.float32)
    return mixed.astype(jnp.bfloat16)


def per_device(tokens, attn_gain, w_query, w_key, w_value, w_out, mlp_gain, w_gate, w_up, w_down):
    rows = tokens.shape[0]
    yl, core = lax.axis_index("yl"), lax.axis_index("c")
    place = lax.axis_index(PLANE)
    plane = lax.axis_size("x") * lax.axis_size("z")
    out_t, down_t = w_out.T, w_down.T
    heads = w_query.shape[1] // 2
    units = w_gate.shape[1] // 2
    padded = -(-units // 128) * 128

    def half(array, h, width):
        return array[:, h * width : (h + 1) * width]

    def wide(array, h):
        return jnp.pad(half(array, h, units), ((0, 0), (0, padded - units)))

    attn_parts = [
        jnp.concatenate(
            [(w_key, w_value)[h], half(w_query, h, heads), half(out_t, h, heads)], axis=1
        )
        for h in range(2)
    ]
    mlp_parts = [
        jnp.concatenate([wide(w_gate, h), wide(w_up, h), wide(down_t, h)], axis=1)
        for h in range(2)
    ]
    attn_rows = shuffled_rows(attn_parts)
    mlp_rows = shuffled_rows(mlp_parts)
    mlp_full = lax.all_gather(mlp_rows, PLANE, axis=0, tiled=True)

    normed = scaled_rows(column_tokens(tokens), attn_gain)
    kv_width = w_key.shape[1]
    kv_full = plane_rows(attn_rows[:, :kv_width])
    fresh = product(normed, kv_full).astype(jnp.bfloat16).reshape(2, rows, kv_width)
    reach = -(-WINDOW // rows)
    context = [fresh]
    for step in range(1, reach + 1):
        came = lax.ppermute(fresh, PLANE, [(i, (i + step) % plane) for i in range(plane)])
        context.insert(0, jnp.where(place < step, came[::-1], came))
    context = jnp.concatenate(context, axis=1)
    keys, values = ordered(core, context, other_core(context))

    rest_z = spread(attn_rows[:, kv_width:], "z")
    rest_z = rest_z.reshape(-1, rest_z.shape[2])
    query_full = spread(rest_z[:, :heads], "x").reshape(-1, heads)
    out_full = spread(rest_z[:, heads:], "x")
    queries = product(normed, query_full).astype(jnp.bfloat16)
    queries = queries.reshape(2, rows, heads // HEAD_DIM, HEAD_DIM)
    runs = jnp.stack([yl, 1 - yl])
    first_key = (runs * plane + place - reach) * rows
    attended = window_attention(queries, keys, values, first_key).reshape(2 * rows, heads)
    attn_share = column_sum(attended, out_full.reshape(4, -1, heads))
    stream_share = (tokens.astype(jnp.float32) + attn_share).astype(jnp.bfloat16)

    stream_normed = scaled_rows(column_tokens(stream_share), mlp_gain)
    gate = product(stream_normed, mlp_full[:, :padded])
    upward = product(stream_normed, mlp_full[:, padded : 2 * padded])
    hidden = (jax.nn.silu(gate) * upward).astype(jnp.bfloat16)
    down_full = mlp_full[:, 2 * padded :]
    mlp_share = column_sum(hidden, down_full.reshape(4, -1, padded))
    return (stream_share.astype(jnp.float32) + mlp_share).astype(jnp.bfloat16)


def solution(mesh):
    split = Mesh(mesh.devices.reshape(2, 4, 8, 2, 2), ("yl", "x", "z", "yh", "c"))
    both = P(SEQ, FEATURES)
    down = P(FEATURES, SEQ)
    placed = (both, P(), both, both, both, down, P(), both, both, down)
    return jax.shard_map(
        per_device, mesh=split, in_specs=placed, out_specs=both, check_vma=False
    )
```

```python
import jax
import jax.numpy as jnp
from jax import lax
from jax.experimental import pallas as pl
from jax.experimental.pallas import tpu as pltpu
from jax.sharding import Mesh
from jax.sharding import PartitionSpec as P

HEAD_DIM = 128
WINDOW = 1024
SEQ = ("yl", "x", "z")
FEATURES = ("yh", "c")
PLANE = ("x", "z")
PARTS = 2


def other_core(value):
    return lax.ppermute(value, "c", [(0, 1), (1, 0)])


def column_partner(value, flip):
    return lax.ppermute(value, ("yl", "yh"), [(i, i ^ flip) for i in range(4)])


def ordered(flag, first, second):
    return jnp.where(flag == 0, first, second), jnp.where(flag == 0, second, first)


def column_rows(sends):
    received = [
        lax.ppermute(send, ("yl", "c"), [(yl * 2 + c, c * 2 + (yl ^ swap)) for yl in range(2) for c in range(2)])
        for swap, send in enumerate(sends)
    ]
    return jnp.stack(ordered(lax.axis_index("c"), *received))


def column_blocks(share):
    blocks = [share]
    for flip in (1, 2, 3):
        blocks.append(column_partner(share, flip))
    mine = jnp.stack(blocks)
    return mine, other_core(mine)


def call(kernel, grid, scalars, in_specs, out_specs, out_shape, scratch=(), flops=0, moved=0):
    return pl.pallas_call(
        kernel,
        grid_spec=pltpu.PrefetchScalarGridSpec(
            num_scalar_prefetch=scalars,
            grid=grid,
            in_specs=in_specs,
            out_specs=out_specs,
            scratch_shapes=scratch,
        ),
        out_shape=out_shape,
        cost_estimate=pl.CostEstimate(flops=flops, bytes_accessed=moved, transcendentals=0),
    )


def store_normed(me_ref, mine_ref, theirs_ref, gain_ref, out_ref, run, at):
    n, f = mine_ref.shape[1:]
    parts = [
        (half * 2 + other, (mine_ref, theirs_ref)[other][run * 2 + half].astype(jnp.float32))
        for half in range(2)
        for other in range(2)
    ]
    squares = sum(jnp.sum(x * x, axis=1, keepdims=True) for _, x in parts)
    scale = lax.rsqrt(squares / (len(parts) * f) + 1e-06)
    for flip, x in parts:
        column = pl.multiple_of((me_ref[0] ^ flip) * f, f)
        gain = gain_ref[:, pl.ds(column, f)]
        out_ref[pl.ds(at, n), pl.ds(column, f)] = (x * scale * gain).astype(jnp.bfloat16)


def normed_rows(me, mine, theirs, gain):
    rows, f = mine.shape[1:]
    step = min(256, rows)

    def kernel(me_ref, mine_ref, theirs_ref, gain_ref, out_ref):
        store_normed(me_ref, mine_ref, theirs_ref, gain_ref, out_ref, 0, 0)

    block = pl.BlockSpec((2, step, f), lambda run, i, me: (run, i, 0))
    tiles = rows // step
    return call(
        kernel,
        (2, tiles),
        1,
        [block, block, pl.BlockSpec((1, 4 * f), lambda run, i, me: (0, 0))],
        pl.BlockSpec((step, 4 * f), lambda run, i, me: (run * tiles + i, 0)),
        jax.ShapeDtypeStruct((2 * rows, 4 * f), jnp.bfloat16),
        flops=rows * f * 100,
        moved=rows * f * 32,
    )(me, mine, theirs, gain[None])


def unit_terms(me, mine, theirs, gain, weights):
    rows, f = mine.shape[1:]
    chips, runs, r = weights.shape[:3]
    d = chips * runs * r
    width = weights.shape[3] // 3
    step = 256
    steps = width // step

    def kernel(
        me_ref, mine_ref, theirs_ref, gain_ref, gate_ref, up_ref, down_ref, near_ref, away_ref,
        normed, total,
    ):
        j = pl.program_id(0)

        @pl.when(j == 0)
        def _():
            for run in range(2):
                store_normed(
                    me_ref, mine_ref, theirs_ref, gain_ref, normed, run, run * rows
                )

        gate = up = 0.0
        for run in range(runs):
            x = normed[:, run * chips * r : (run + 1) * chips * r]
            gate_rows = gate_ref[:, run].reshape(chips * r, step)
            gate = gate + jnp.dot(x, gate_rows, preferred_element_type=jnp.float32)
            up_rows = up_ref[:, run].reshape(chips * r, step)
            up = up + jnp.dot(x, up_rows, preferred_element_type=jnp.float32)
        hidden = (gate / (1.0 + jnp.exp(-gate)) * up).astype(jnp.bfloat16)
        for place, flip in enumerate((1, 3, 0, 2)):
            term = lax.dot_general(
                hidden,
                feature_rows(down_ref, me_ref[0] ^ flip),
                (((1,), (1,)), ((), ())),
                preferred_element_type=jnp.float32,
            )
            out = total if place < 2 else near_ref
            cols = slice(place % 2 * f, (place % 2 + 1) * f)

            @pl.when(j == 0)
            def _():
                out[:, cols] = term

            @pl.when(j > 0)
            def _():
                out[:, cols] += term

        @pl.when(j == steps - 1)
        def _():
            away_ref[...] = total[...].astype(jnp.bfloat16)

    def whole(shape):
        return pl.BlockSpec(shape, lambda j, me: (0,) * len(shape))

    def weight(part):
        return pl.BlockSpec((chips, runs, r, step), lambda j, me: (0, 0, 0, part * steps + j))

    shape = (2 * rows, 2 * f)
    return call(
        kernel,
        (steps,),
        1,
        [whole(mine.shape), whole(mine.shape), whole((1, 4 * f))]
        + [weight(part) for part in range(3)],
        [whole(shape), whole(shape)],
        [jax.ShapeDtypeStruct(shape, jnp.float32), jax.ShapeDtypeStruct(shape, jnp.bfloat16)],
        [pltpu.VMEM((2 * rows, 4 * f), jnp.bfloat16), pltpu.VMEM(shape, jnp.float32)],
        flops=2 * 2 * rows * width * (2 * d + 4 * f),
        moved=2 * weights.size + 16 * rows * f * 2,
    )(me, mine, theirs, gain[None], weights, weights, weights)


def projected(left, weights, start, width):
    n, d = left.shape
    chips, runs, r = weights.shape[:3]
    step = 512

    def kernel(x_ref, w_ref, out_ref):
        total = 0.0
        for run in range(runs):
            w = w_ref[:, run].reshape(chips * r, width)
            x = x_ref[:, run * chips * r : (run + 1) * chips * r]
            total = total + jnp.dot(x, w, preferred_element_type=jnp.float32)
        out_ref[...] = total.astype(jnp.bfloat16)

    return call(
        kernel,
        (n // step,),
        0,
        [
            pl.BlockSpec((step, d), lambda i: (i, 0)),
            pl.BlockSpec((chips, runs, r, width), lambda i: (0, 0, 0, start // width)),
        ],
        pl.BlockSpec((step, width), lambda i: (i, 0)),
        jax.ShapeDtypeStruct((n, width), jnp.bfloat16),
        flops=2 * n * d * width,
        moved=2 * (n * d + d * width + n * width),
    )(left, weights)


def feature_rows(weights_ref, block):
    chips, _, r, k = weights_ref.shape
    half = chips // 2
    at = pl.multiple_of(lax.rem(block, 2) * half, half)
    return weights_ref[pl.ds(at, half), lax.div(block, 2)].reshape(half * r, k)


def head_terms(me, attended, weights, part):
    rows, width = attended.shape[1] // PARTS, attended.shape[2]
    f = weights.shape[0] * weights.shape[1] * weights.shape[2] // 4

    def kernel(me_ref, left_ref, weights_ref, near_ref, away_ref):
        left = left_ref[...].reshape(2 * rows, width)
        for place, flip in enumerate((1, 3, 0, 2)):
            term = lax.dot_general(
                left,
                feature_rows(weights_ref, me_ref[0] ^ flip),
                (((1,), (1,)), ((), ())),
                preferred_element_type=jnp.float32,
            )
            out = away_ref if place < 2 else near_ref
            out[:, place % 2 * f : (place % 2 + 1) * f] = term.astype(out.dtype)

    shape = (2 * rows, 2 * f)
    whole = pl.BlockSpec(shape, lambda i, me: (0, 0))
    return call(
        kernel,
        (1,),
        1,
        [
            pl.BlockSpec((2, rows, width), lambda i, me: (0, part, 0)),
            pl.BlockSpec((*weights.shape[:3], width), lambda i, me: (0, 0, 0, 1)),
        ],
        [whole, whole],
        [jax.ShapeDtypeStruct(shape, jnp.float32), jax.ShapeDtypeStruct(shape, jnp.bfloat16)],
        flops=4 * rows * 4 * f * width,
        moved=8 * f * width + 24 * rows * f,
    )(me, attended, weights)


def column_sum(near, away):
    rows, f = near.shape[0] // 2, near.shape[1] // 2
    both = near + other_core(away).astype(jnp.float32)
    total = both[:rows, :f]
    sent = (
        (both[:rows, f:], 1),
        (both[rows:, :f], 2),
        (both[rows:, f:], 3),
    )
    for value, flip in sent:
        total = total + column_partner(value.astype(jnp.bfloat16), flip).astype(jnp.float32)
    return total


def window_attention(queries, keys, values, first_key):
    rows, width = queries.shape[1:]
    span = keys.shape[1]
    count = width // HEAD_DIM
    step = min(256, rows)
    seen = WINDOW + step
    scale = HEAD_DIM ** (-0.5)

    def kernel(first_ref, q_ref, k_ref, v_ref, out_ref):
        run, tile = pl.program_id(0), pl.program_id(1)
        start = pl.multiple_of(tile * step + span - rows - WINDOW, step)
        k = k_ref[0, pl.ds(start, seen), :]
        v = v_ref[0, pl.ds(start, seen), :]
        query_pos = lax.broadcasted_iota(jnp.int32, (step, seen), 0)
        key_pos = lax.broadcasted_iota(jnp.int32, (step, seen), 1)
        distance = query_pos + WINDOW - key_pos
        allowed = (distance >= 0) & (distance < WINDOW)
        allowed = allowed & (key_pos >= -first_ref[run] - start)
        for head in range(count):
            cols = slice(head * HEAD_DIM, (head + 1) * HEAD_DIM)
            scores = lax.dot_general(
                q_ref[0, :, cols], k, (((1,), (1,)), ((), ())), preferred_element_type=jnp.float32
            )
            scores = jnp.where(allowed, scores * scale, -1e30)
            raised = jnp.exp(scores - jnp.max(scores, axis=1, keepdims=True))
            total = jnp.sum(raised, axis=1, keepdims=True)
            mixed = jnp.dot(raised.astype(jnp.bfloat16), v, preferred_element_type=jnp.float32)
            out_ref[0, :, cols] = (mixed / total).astype(jnp.bfloat16)

    whole = pl.BlockSpec((1, span, HEAD_DIM), lambda run, tile, first: (run, 0, 0))
    part = pl.BlockSpec((1, step, width), lambda run, tile, first: (run, tile, 0))
    return call(
        kernel,
        (2, rows // step),
        1,
        [part, whole, whole],
        part,
        jax.ShapeDtypeStruct(queries.shape, jnp.bfloat16),
        flops=2 * rows * width * seen * 4,
        moved=2 * (2 * queries.size + keys.size + values.size),
    )(first_key, queries, keys, values)


def packed(parity, parts):
    arrays = [array for part in parts for array, *_ in part]
    rows = arrays[0].shape[0]
    width = sum(-(-size // 128) * 128 for _, _, size in parts[0])

    def kernel(parity_ref, *refs):
        ins, outs = refs[:-2], refs[-2:]
        for swap in range(2):

            @pl.when(parity_ref[0] == swap)
            def _():
                for h in range(2):
                    out = outs[h ^ swap]
                    at = 0
                    for i, (_, start, size) in enumerate(parts[h]):
                        ref = ins[h * len(parts[0]) + i]
                        out[:, at : at + size] = ref[:, start : start + size]
                        full = -(-size // 128) * 128
                        if full > size:
                            out[:, at + size : at + full] = jnp.zeros(
                                (rows, full - size), jnp.bfloat16
                            )
                        at += full

    def spec(shape):
        return pl.BlockSpec(shape, lambda i, parity: (0, 0))

    return call(
        kernel,
        (1,),
        1,
        [spec(array.shape) for array in arrays],
        [spec((rows, width))] * 2,
        [jax.ShapeDtypeStruct((rows, width), jnp.bfloat16)] * 2,
        moved=8 * rows * width,
    )(parity, *arrays)


def per_device(tokens, attn_gain, w_query, w_key, w_value, w_out, mlp_gain, w_gate, w_up, w_down):
    rows = tokens.shape[0]
    yl, yh, core = (lax.axis_index(name) for name in ("yl", "yh", "c"))
    place = lax.axis_index(PLANE)
    plane = lax.axis_size("x") * lax.axis_size("z")
    me = jnp.reshape(yh * 2 + core, (1,)).astype(jnp.int32)
    parity = jnp.reshape(yl, (1,)).astype(jnp.int32)
    out_t, down_t = w_out.T, w_down.T
    kv_width = w_key.shape[1]
    heads = w_query.shape[1] // 2
    units = w_gate.shape[1] // 2

    attn_rows = column_rows(
        packed(
            parity,
            [
                [
                    (w_query, h * heads, heads),
                    (out_t, h * heads, heads),
                    ((w_key, w_value)[h], 0, kv_width),
                ]
                for h in range(2)
            ],
        )
    )
    attn_full = lax.all_gather(attn_rows[None], "z", axis=0, tiled=True)
    mlp_rows = column_rows(
        packed(
            parity,
            [[(array, h * units, units) for array in (w_gate, w_up, down_t)] for h in range(2)],
        )
    )
    attn_full = lax.all_gather(attn_full, "x", axis=0, tiled=True)
    normed = normed_rows(me, *column_blocks(tokens), attn_gain)
    mlp_rows, attn_full, normed = lax.optimization_barrier((mlp_rows, attn_full, normed))
    mlp_full = lax.all_gather(mlp_rows[None], PLANE, axis=0, tiled=True)
    fresh = projected(normed, attn_full, 2 * heads, kv_width).reshape(2, rows, kv_width)
    reach = -(-WINDOW // rows)
    context = [fresh]
    for step in range(1, reach + 1):
        came = lax.ppermute(fresh, PLANE, [(i, (i + step) % plane) for i in range(plane)])
        context.insert(0, jnp.where(place < step, came[::-1], came))
    context = jnp.concatenate(context, axis=1)
    keys, values = ordered(core, context, other_core(context))

    queries = projected(normed, attn_full, 0, heads).reshape(2, rows, heads)
    runs = jnp.stack([yl, 1 - yl])
    first_key = ((runs * plane + place - reach) * rows).astype(jnp.int32)
    attended = window_attention(queries, keys, values, first_key)
    part = rows // PARTS
    outputs = []
    for at in range(0, rows, part):
        attn_share = column_sum(*head_terms(me, attended, attn_full, at // part))
        stream = tokens[at : at + part].astype(jnp.float32) + attn_share
        stream = stream.astype(jnp.bfloat16)
        terms = unit_terms(me, *column_blocks(stream), mlp_gain, mlp_full)
        outputs.append((stream.astype(jnp.float32) + column_sum(*terms)).astype(jnp.bfloat16))
    return jnp.concatenate(outputs, axis=0)


def solution(mesh):
    split = Mesh(mesh.devices.reshape(2, 4, 8, 2, 2), ("yl", "x", "z", "yh", "c"))
    both = P(SEQ, FEATURES)
    down = P(FEATURES, SEQ)
    placed = (both, P(), both, both, both, down, P(), both, both, down)

    return jax.shard_map(per_device, mesh=split, in_specs=placed, out_specs=both, check_vma=False)
```

```python
import jax
import jax.numpy as jnp
from jax import lax
from jax.experimental import pallas as pl
from jax.experimental.pallas import tpu as pltpu
from jax.sharding import Mesh
from jax.sharding import PartitionSpec as P

HEAD_DIM = 128
WINDOW = 1024
SEQ = ("yl", "x", "z")
FEATURES = ("yh", "c")
PLANE = ("x", "z")
PARTS = 2


def spread(value, axis):
    length = lax.axis_size(axis)
    return lax.all_to_all(
        jnp.broadcast_to(value[None], (length, *value.shape)), axis, 0, 0, tiled=True
    )


def other_core(value):
    return lax.ppermute(value, "c", [(0, 1), (1, 0)])


def column_partner(value, flip):
    return lax.ppermute(value, ("yl", "yh"), [(i, i ^ flip) for i in range(4)])


def ordered(flag, first, second):
    return jnp.where(flag == 0, first, second), jnp.where(flag == 0, second, first)


def column_rows(sends):
    received = [
        lax.ppermute(send, ("yl", "c"), [(yl * 2 + c, c * 2 + (yl ^ swap)) for yl in range(2) for c in range(2)])
        for swap, send in enumerate(sends)
    ]
    return jnp.stack(ordered(lax.axis_index("c"), *received))


def column_blocks(share):
    blocks = [share]
    for flip in (1, 2, 3):
        blocks.append(column_partner(share, flip))
    mine = jnp.stack(blocks)
    return mine, other_core(mine)


def call(kernel, grid, scalars, in_specs, out_specs, out_shape, scratch=(), flops=0, moved=0):
    return pl.pallas_call(
        kernel,
        grid_spec=pltpu.PrefetchScalarGridSpec(
            num_scalar_prefetch=scalars,
            grid=grid,
            in_specs=in_specs,
            out_specs=out_specs,
            scratch_shapes=scratch,
        ),
        out_shape=out_shape,
        cost_estimate=pl.CostEstimate(flops=flops, bytes_accessed=moved, transcendentals=0),
    )


def store_normed(me_ref, mine_ref, theirs_ref, gain_ref, out_ref, run, at):
    n, f = mine_ref.shape[1:]
    parts = [
        (half * 2 + other, (mine_ref, theirs_ref)[other][run * 2 + half].astype(jnp.float32))
        for half in range(2)
        for other in range(2)
    ]
    squares = sum(jnp.sum(x * x, axis=1, keepdims=True) for _, x in parts)
    scale = lax.rsqrt(squares / (len(parts) * f) + 1e-06)
    for flip, x in parts:
        column = pl.multiple_of((me_ref[0] ^ flip) * f, f)
        gain = gain_ref[:, pl.ds(column, f)]
        out_ref[pl.ds(at, n), pl.ds(column, f)] = (x * scale * gain).astype(jnp.bfloat16)


def normed_rows(me, mine, theirs, gain):
    rows, f = mine.shape[1:]
    step = min(256, rows)

    def kernel(me_ref, mine_ref, theirs_ref, gain_ref, out_ref):
        store_normed(me_ref, mine_ref, theirs_ref, gain_ref, out_ref, 0, 0)

    block = pl.BlockSpec((2, step, f), lambda run, i, me: (run, i, 0))
    tiles = rows // step
    return call(
        kernel,
        (2, tiles),
        1,
        [block, block, pl.BlockSpec((1, 4 * f), lambda run, i, me: (0, 0))],
        pl.BlockSpec((step, 4 * f), lambda run, i, me: (run * tiles + i, 0)),
        jax.ShapeDtypeStruct((2 * rows, 4 * f), jnp.bfloat16),
        flops=rows * f * 100,
        moved=rows * f * 32,
    )(me, mine, theirs, gain[None])


def unit_terms(me, mine, theirs, gain, weights):
    rows, f = mine.shape[1:]
    chips, runs, r = weights.shape[:3]
    d = chips * runs * r
    width = weights.shape[3] // 3
    step = 256
    steps = width // step

    def kernel(
        me_ref, mine_ref, theirs_ref, gain_ref, gate_ref, up_ref, all_ref, near_ref, away_ref,
        normed, hidden, down_ref, arrived,
    ):
        j = pl.program_id(0)
        fetch = pltpu.make_async_copy(all_ref.at[:, :, :, 2 * width :], down_ref, arrived)

        @pl.when(j == 0)
        def _():
            fetch.start()
            for run in range(2):
                store_normed(
                    me_ref, mine_ref, theirs_ref, gain_ref, normed, run, run * rows
                )

        @pl.when(j < steps)
        def _():
            gate = up = 0.0
            for run in range(runs):
                x = normed[:, run * chips * r : (run + 1) * chips * r]
                gate_rows = gate_ref[:, run].reshape(chips * r, step)
                gate = gate + jnp.dot(x, gate_rows, preferred_element_type=jnp.float32)
                up_rows = up_ref[:, run].reshape(chips * r, step)
                up = up + jnp.dot(x, up_rows, preferred_element_type=jnp.float32)
            hidden[j] = (gate / (1.0 + jnp.exp(-gate)) * up).astype(jnp.bfloat16)

        @pl.when(j == steps)
        def _():
            fetch.wait()

        @pl.when(j >= steps)
        def _():
            left = jnp.concatenate([hidden[i] for i in range(steps)], axis=1)
            for out, flip in ((away_ref, 2 * (j - steps) + 1), (near_ref, 2 * (j - steps))):
                term = lax.dot_general(
                    left,
                    feature_rows(down_ref, me_ref[0] ^ flip),
                    (((1,), (1,)), ((), ())),
                    preferred_element_type=jnp.float32,
                )
                out[...] = term.astype(out.dtype)

    def whole(shape):
        return pl.BlockSpec(shape, lambda j, me: (0,) * len(shape))

    def weight(part):
        return pl.BlockSpec(
            (chips, runs, r, step),
            lambda j, me: (0, 0, 0, part * steps + jnp.minimum(j, steps - 1)),
        )

    shape = (2 * rows, 2 * f)
    return call(
        kernel,
        (steps + 2,),
        1,
        [whole(mine.shape), whole(mine.shape), whole((1, 4 * f))]
        + [weight(0), weight(1), pl.BlockSpec(memory_space=pl.ANY)],
        [pl.BlockSpec((2 * rows, f), lambda j, me: (0, jnp.maximum(j - steps, 0)))] * 2,
        [jax.ShapeDtypeStruct(shape, jnp.float32), jax.ShapeDtypeStruct(shape, jnp.bfloat16)],
        [
            pltpu.VMEM((2 * rows, 4 * f), jnp.bfloat16),
            pltpu.VMEM((steps, 2 * rows, step), jnp.bfloat16),
            pltpu.VMEM((chips, runs, r, width), jnp.bfloat16),
            pltpu.SemaphoreType.DMA,
        ],
        flops=2 * 2 * rows * width * (2 * d + 4 * f),
        moved=2 * weights.size + 16 * rows * f * 2,
    )(me, mine, theirs, gain[None], weights, weights, weights)


def projected(left, weights, start, width):
    n, d = left.shape
    chips, runs, r = weights.shape[:3]
    step = 512

    def kernel(x_ref, w_ref, out_ref):
        total = 0.0
        for run in range(runs):
            w = w_ref[:, run].reshape(chips * r, width)
            x = x_ref[:, run * chips * r : (run + 1) * chips * r]
            total = total + jnp.dot(x, w, preferred_element_type=jnp.float32)
        out_ref[...] = total.astype(jnp.bfloat16)

    return call(
        kernel,
        (n // step,),
        0,
        [
            pl.BlockSpec((step, d), lambda i: (i, 0)),
            pl.BlockSpec((chips, runs, r, width), lambda i: (0, 0, 0, start // width)),
        ],
        pl.BlockSpec((step, width), lambda i: (i, 0)),
        jax.ShapeDtypeStruct((n, width), jnp.bfloat16),
        flops=2 * n * d * width,
        moved=2 * (n * d + d * width + n * width),
    )(left, weights)


def feature_rows(weights_ref, block):
    chips, _, r, k = weights_ref.shape
    half = chips // 2
    at = pl.multiple_of(lax.rem(block, 2) * half, half)
    return weights_ref[pl.ds(at, half), lax.div(block, 2)].reshape(half * r, k)


def head_terms(me, attended, weights):
    rows, width = attended.shape[1:]
    f = weights.shape[0] * weights.shape[1] * weights.shape[2] // 4

    def kernel(me_ref, left_ref, weights_ref, near_ref, away_ref):
        left = left_ref[...].reshape(2 * rows, width)
        at = 2 * pl.program_id(0)
        for out, flip in ((away_ref, at + 1), (near_ref, at)):
            term = lax.dot_general(
                left,
                feature_rows(weights_ref, me_ref[0] ^ flip),
                (((1,), (1,)), ((), ())),
                preferred_element_type=jnp.float32,
            )
            out[...] = term.astype(out.dtype)

    shape = (2 * rows, 2 * f)
    return call(
        kernel,
        (2,),
        1,
        [
            pl.BlockSpec((2, rows, width), lambda i, me: (0, 0, 0)),
            pl.BlockSpec((*weights.shape[:3], width), lambda i, me: (0, 0, 0, 0)),
        ],
        [pl.BlockSpec((2 * rows, f), lambda i, me: (0, i))] * 2,
        [jax.ShapeDtypeStruct(shape, jnp.float32), jax.ShapeDtypeStruct(shape, jnp.bfloat16)],
        flops=4 * rows * 4 * f * width,
        moved=8 * f * width + 24 * rows * f,
    )(me, attended, weights)


def column_sum(near, away):
    rows, f = near.shape[0] // 2, near.shape[1] // 2
    both = near + other_core(away).astype(jnp.float32)
    total = both[:rows, :f]
    sent = (
        (both[:rows, f:], 1),
        (both[rows:, :f], 2),
        (both[rows:, f:], 3),
    )
    for value, flip in sent:
        came = column_partner(value.astype(jnp.bfloat16), flip)
        total = total + came.astype(jnp.float32)
    return total


def window_attention(queries, keys, values, first_key, part):
    rows, width = queries.shape[1:]
    span = keys.shape[1]
    count = width // HEAD_DIM
    step = rows // PARTS
    seen = WINDOW + step
    start = part * step + span - rows - WINDOW
    scale = HEAD_DIM ** (-0.5)

    def kernel(first_ref, q_ref, k_ref, v_ref, out_ref):
        run = pl.program_id(0)
        k = k_ref[0, start : start + seen, :]
        v = v_ref[0, start : start + seen, :]
        query_pos = lax.broadcasted_iota(jnp.int32, (step, seen), 0)
        key_pos = lax.broadcasted_iota(jnp.int32, (step, seen), 1)
        distance = query_pos + WINDOW - key_pos
        allowed = (distance >= 0) & (distance < WINDOW)
        allowed = allowed & (key_pos >= -first_ref[run] - start)
        for head in range(count):
            cols = slice(head * HEAD_DIM, (head + 1) * HEAD_DIM)
            scores = lax.dot_general(
                q_ref[0, :, cols], k, (((1,), (1,)), ((), ())), preferred_element_type=jnp.float32
            )
            scores = jnp.where(allowed, scores * scale, -1e30)
            raised = jnp.exp(scores - jnp.max(scores, axis=1, keepdims=True))
            total = jnp.sum(raised, axis=1, keepdims=True)
            mixed = jnp.dot(raised.astype(jnp.bfloat16), v, preferred_element_type=jnp.float32)
            out_ref[0, :, cols] = (mixed / total).astype(jnp.bfloat16)

    whole = pl.BlockSpec((1, span, HEAD_DIM), lambda run, first: (run, 0, 0))
    return call(
        kernel,
        (2,),
        1,
        [pl.BlockSpec((1, step, width), lambda run, first: (run, part, 0)), whole, whole],
        pl.BlockSpec((1, step, width), lambda run, first: (run, 0, 0)),
        jax.ShapeDtypeStruct((2, step, width), jnp.bfloat16),
        flops=2 * step * width * seen * 4,
        moved=2 * (2 * queries.size // PARTS + keys.size + values.size),
    )(first_key, queries, keys, values)


def packed(parity, parts):
    arrays = [array for part in parts for array, *_ in part]
    rows = arrays[0].shape[0]
    width = sum(-(-size // 128) * 128 for _, _, size in parts[0])

    def kernel(parity_ref, *refs):
        ins, outs = refs[:-2], refs[-2:]
        for swap in range(2):

            @pl.when(parity_ref[0] == swap)
            def _():
                for h in range(2):
                    out = outs[h ^ swap]
                    at = 0
                    for i, (_, start, size) in enumerate(parts[h]):
                        ref = ins[h * len(parts[0]) + i]
                        out[:, at : at + size] = ref[:, start : start + size]
                        full = -(-size // 128) * 128
                        if full > size:
                            out[:, at + size : at + full] = jnp.zeros(
                                (rows, full - size), jnp.bfloat16
                            )
                        at += full

    def spec(shape):
        return pl.BlockSpec(shape, lambda i, parity: (0, 0))

    return call(
        kernel,
        (1,),
        1,
        [spec(array.shape) for array in arrays],
        [spec((rows, width))] * 2,
        [jax.ShapeDtypeStruct((rows, width), jnp.bfloat16)] * 2,
        moved=8 * rows * width,
    )(parity, *arrays)


def per_device(tokens, attn_gain, w_query, w_key, w_value, w_out, mlp_gain, w_gate, w_up, w_down):
    rows = tokens.shape[0]
    yl, yh, core = (lax.axis_index(name) for name in ("yl", "yh", "c"))
    place = lax.axis_index(PLANE)
    plane = lax.axis_size("x") * lax.axis_size("z")
    me = jnp.reshape(yh * 2 + core, (1,)).astype(jnp.int32)
    parity = jnp.reshape(yl, (1,)).astype(jnp.int32)
    out_t, down_t = w_out.T, w_down.T
    kv_width = w_key.shape[1]
    heads = w_query.shape[1] // 2
    units = w_gate.shape[1] // 2

    attn_rows = column_rows(
        packed(
            parity,
            [
                [
                    (w_query, h * heads, heads),
                    ((w_key, w_value)[h], 0, kv_width),
                    (out_t, h * heads, heads),
                ]
                for h in range(2)
            ],
        )
    )
    split = heads + kv_width
    attn_full = spread(attn_rows, "z")
    attn_full, out_full = attn_full[..., :split], attn_full[..., split:]
    mlp_rows = column_rows(
        packed(
            parity,
            [[(array, h * units, units) for array in (w_gate, w_up, down_t)] for h in range(2)],
        )
    )
    attn_full = lax.all_gather(attn_full, "x", axis=0, tiled=True)
    normed = normed_rows(me, *column_blocks(tokens), attn_gain)
    mlp_rows, attn_full, normed = lax.optimization_barrier((mlp_rows, attn_full, normed))
    mlp_full = lax.all_gather(mlp_rows[None], PLANE, axis=0, tiled=True)
    out_full = spread(out_full, "x")
    out_full = out_full.reshape(-1, *out_full.shape[2:])
    fresh = projected(normed, attn_full, heads, kv_width).reshape(2, rows, kv_width)
    reach = -(-WINDOW // rows)
    context = [fresh]
    for step in range(1, reach + 1):
        came = lax.ppermute(fresh, PLANE, [(i, (i + step) % plane) for i in range(plane)])
        context.insert(0, jnp.where(place < step, came[::-1], came))
    context = jnp.concatenate(context, axis=1)
    keys, values = ordered(core, context, other_core(context))

    queries = projected(normed, attn_full, 0, heads).reshape(2, rows, heads)
    runs = jnp.stack([yl, 1 - yl])
    first_key = ((runs * plane + place - reach) * rows).astype(jnp.int32)
    part = rows // PARTS
    outputs = []
    for i in range(PARTS):
        attended = window_attention(queries, keys, values, first_key, i)
        attn_share = column_sum(*head_terms(me, attended, out_full))
        residual = tokens[i * part : (i + 1) * part]
        if i > 0:
            residual, stream = lax.optimization_barrier((residual, stream))
        stream = (residual.astype(jnp.float32) + attn_share).astype(jnp.bfloat16)
        blocks = column_blocks(stream)
        terms = unit_terms(me, *blocks, mlp_gain, mlp_full)
        mlp_share = column_sum(*terms)
        outputs.append((stream.astype(jnp.float32) + mlp_share).astype(jnp.bfloat16))
    return jnp.concatenate(outputs, axis=0)


def solution(mesh):
    split = Mesh(mesh.devices.reshape(2, 4, 8, 2, 2), ("yl", "x", "z", "yh", "c"))
    both = P(SEQ, FEATURES)
    down = P(FEATURES, SEQ)
    placed = (both, P(), both, both, both, down, P(), both, both, down)

    return jax.shard_map(per_device, mesh=split, in_specs=placed, out_specs=both, check_vma=False)
```

```python
import jax
import jax.numpy as jnp
from jax import lax
from jax.experimental import pallas as pl
from jax.experimental.pallas import tpu as pltpu
from jax.sharding import Mesh
from jax.sharding import PartitionSpec as P

HEAD_DIM = 128
WINDOW = 1024
SEQ = ("yl", "x", "z")
FEATURES = ("yh", "c")
PLANE = ("x", "z")
PARTS = 2


def spread(value, axis):
    length = lax.axis_size(axis)
    return lax.all_to_all(
        jnp.broadcast_to(value[None], (length, *value.shape)), axis, 0, 0, tiled=True
    )


def other_core(value):
    return lax.ppermute(value, "c", [(0, 1), (1, 0)])


def column_partner(value, flip):
    return lax.ppermute(value, ("yl", "yh"), [(i, i ^ flip) for i in range(4)])


def ordered(flag, first, second):
    return jnp.where(flag == 0, first, second), jnp.where(flag == 0, second, first)


def column_rows(sends):
    received = [
        lax.ppermute(send, ("yl", "c"), [(yl * 2 + c, c * 2 + (yl ^ swap)) for yl in range(2) for c in range(2)])
        for swap, send in enumerate(sends)
    ]
    return jnp.stack(ordered(lax.axis_index("c"), *received))


def column_blocks(share):
    blocks = [share]
    for flip in (1, 2, 3):
        blocks.append(column_partner(share, flip))
    mine = jnp.stack(blocks)
    return mine, other_core(mine)


def call(kernel, grid, scalars, in_specs, out_specs, out_shape, scratch=(), flops=0, moved=0):
    return pl.pallas_call(
        kernel,
        grid_spec=pltpu.PrefetchScalarGridSpec(
            num_scalar_prefetch=scalars,
            grid=grid,
            in_specs=in_specs,
            out_specs=out_specs,
            scratch_shapes=scratch,
        ),
        out_shape=out_shape,
        compiler_params=pltpu.CompilerParams(vmem_limit_bytes=32 * 1024 * 1024),
        cost_estimate=pl.CostEstimate(flops=flops, bytes_accessed=moved, transcendentals=0),
    )


def store_normed(me_ref, mine_ref, theirs_ref, gain_ref, out_ref, run, at):
    n, f = mine_ref.shape[1:]
    parts = [
        (half * 2 + other, (mine_ref, theirs_ref)[other][run * 2 + half].astype(jnp.float32))
        for half in range(2)
        for other in range(2)
    ]
    squares = sum(jnp.sum(x * x, axis=1, keepdims=True) for _, x in parts)
    scale = lax.rsqrt(squares / (len(parts) * f) + 1e-06)
    for flip, x in parts:
        column = pl.multiple_of((me_ref[0] ^ flip) * f, f)
        gain = gain_ref[:, pl.ds(column, f)]
        out_ref[pl.ds(at, n), pl.ds(column, f)] = (x * scale * gain).astype(jnp.bfloat16)


def normed_rows(me, mine, theirs, gain):
    rows, f = mine.shape[1:]
    step = min(256, rows)

    def kernel(me_ref, mine_ref, theirs_ref, gain_ref, out_ref):
        store_normed(me_ref, mine_ref, theirs_ref, gain_ref, out_ref, 0, 0)

    block = pl.BlockSpec((2, step, f), lambda run, i, me: (run, i, 0))
    tiles = rows // step
    return call(
        kernel,
        (2, tiles),
        1,
        [block, block, pl.BlockSpec((1, 4 * f), lambda run, i, me: (0, 0))],
        pl.BlockSpec((step, 4 * f), lambda run, i, me: (run * tiles + i, 0)),
        jax.ShapeDtypeStruct((2 * rows, 4 * f), jnp.bfloat16),
        flops=rows * f * 100,
        moved=rows * f * 32,
    )(me, mine, theirs, gain[None])


def unit_terms(me, mine, theirs, gain, weights):
    rows, f = mine.shape[1:]
    chips, runs, r = weights.shape[:3]
    d = chips * runs * r
    width = weights.shape[3] // 3
    step = 256
    steps = width // step

    def kernel(
        me_ref, mine_ref, theirs_ref, gain_ref, gate_ref, up_ref, all_ref, near_ref, away_ref,
        normed, hidden, down_ref, arrived,
    ):
        j = pl.program_id(0)
        fetch = pltpu.make_async_copy(all_ref.at[:, :, :, 2 * width :], down_ref, arrived)

        @pl.when(j == 0)
        def _():
            fetch.start()
            for run in range(2):
                store_normed(
                    me_ref, mine_ref, theirs_ref, gain_ref, normed, run, run * rows
                )

        @pl.when(j < steps)
        def _():
            gate = up = 0.0
            for run in range(runs):
                x = normed[:, run * chips * r : (run + 1) * chips * r]
                gate_rows = gate_ref[:, run].reshape(chips * r, step)
                gate = gate + jnp.dot(x, gate_rows, preferred_element_type=jnp.float32)
                up_rows = up_ref[:, run].reshape(chips * r, step)
                up = up + jnp.dot(x, up_rows, preferred_element_type=jnp.float32)
            hidden[j] = (gate / (1.0 + jnp.exp(-gate)) * up).astype(jnp.bfloat16)

        @pl.when(j == steps)
        def _():
            fetch.wait()

        @pl.when(j >= steps)
        def _():
            left = jnp.concatenate([hidden[i] for i in range(steps)], axis=1)
            for out, flip in ((away_ref, 2 * (j - steps) + 1), (near_ref, 2 * (j - steps))):
                term = lax.dot_general(
                    left,
                    feature_rows(down_ref, me_ref[0] ^ flip),
                    (((1,), (1,)), ((), ())),
                    preferred_element_type=jnp.float32,
                )
                out[...] = term.astype(out.dtype)

    def whole(shape):
        return pl.BlockSpec(shape, lambda j, me: (0,) * len(shape))

    def weight(part):
        return pl.BlockSpec(
            (chips, runs, r, step),
            lambda j, me: (0, 0, 0, part * steps + jnp.minimum(j, steps - 1)),
        )

    shape = (2 * rows, 2 * f)
    return call(
        kernel,
        (steps + 2,),
        1,
        [whole(mine.shape), whole(mine.shape), whole((1, 4 * f))]
        + [weight(0), weight(1), pl.BlockSpec(memory_space=pl.ANY)],
        [pl.BlockSpec((2 * rows, f), lambda j, me: (0, jnp.maximum(j - steps, 0)))] * 2,
        [jax.ShapeDtypeStruct(shape, jnp.float32), jax.ShapeDtypeStruct(shape, jnp.bfloat16)],
        [
            pltpu.VMEM((2 * rows, 4 * f), jnp.bfloat16),
            pltpu.VMEM((steps, 2 * rows, step), jnp.bfloat16),
            pltpu.VMEM((chips, runs, r, width), jnp.bfloat16),
            pltpu.SemaphoreType.DMA,
        ],
        flops=2 * 2 * rows * width * (2 * d + 4 * f),
        moved=2 * weights.size + 16 * rows * f * 2,
    )(me, mine, theirs, gain[None], weights, weights, weights)


def projected(left, weights, start, width):
    n, d = left.shape
    chips, runs, r = weights.shape[:3]
    step = 256

    def kernel(x_ref, w_ref, out_ref):
        total = 0.0
        for run in range(runs):
            w = w_ref[:, run].reshape(chips * r, width)
            x = x_ref[:, run * chips * r : (run + 1) * chips * r]
            total = total + jnp.dot(x, w, preferred_element_type=jnp.float32)
        out_ref[...] = total.astype(jnp.bfloat16)

    return call(
        kernel,
        (n // step,),
        0,
        [
            pl.BlockSpec((step, d), lambda i: (i, 0)),
            pl.BlockSpec((chips, runs, r, width), lambda i: (0, 0, 0, start // width)),
        ],
        pl.BlockSpec((step, width), lambda i: (i, 0)),
        jax.ShapeDtypeStruct((n, width), jnp.bfloat16),
        flops=2 * n * d * width,
        moved=2 * (n * d + d * width + n * width),
    )(left, weights)


def feature_rows(weights_ref, block):
    chips, _, r, k = weights_ref.shape
    half = chips // 2
    at = pl.multiple_of(lax.rem(block, 2) * half, half)
    return weights_ref[pl.ds(at, half), lax.div(block, 2)].reshape(half * r, k)


def head_terms(me, attended, weights):
    rows, width = attended.shape[1:]
    f = weights.shape[0] * weights.shape[1] * weights.shape[2] // 4

    def kernel(me_ref, left_ref, weights_ref, near_ref, away_ref):
        left = left_ref[...].reshape(2 * rows, width)
        at = 2 * pl.program_id(0)
        for out, flip in ((away_ref, at + 1), (near_ref, at)):
            term = lax.dot_general(
                left,
                feature_rows(weights_ref, me_ref[0] ^ flip),
                (((1,), (1,)), ((), ())),
                preferred_element_type=jnp.float32,
            )
            out[...] = term.astype(out.dtype)

    shape = (2 * rows, 2 * f)
    return call(
        kernel,
        (2,),
        1,
        [
            pl.BlockSpec((2, rows, width), lambda i, me: (0, 0, 0)),
            pl.BlockSpec((*weights.shape[:3], width), lambda i, me: (0, 0, 0, 0)),
        ],
        [pl.BlockSpec((2 * rows, f), lambda i, me: (0, i))] * 2,
        [jax.ShapeDtypeStruct(shape, jnp.float32), jax.ShapeDtypeStruct(shape, jnp.bfloat16)],
        flops=4 * rows * 4 * f * width,
        moved=8 * f * width + 24 * rows * f,
    )(me, attended, weights)


def column_sum(near, away):
    rows, f = near.shape[0] // 2, near.shape[1] // 2
    both = near + other_core(away).astype(jnp.float32)
    total = both[:rows, :f]
    sent = (
        (both[:rows, f:], 1),
        (both[rows:, :f], 2),
        (both[rows:, f:], 3),
    )
    for value, flip in sent:
        came = column_partner(value.astype(jnp.bfloat16), flip)
        total = total + came.astype(jnp.float32)
    return total


def window_attention(queries, context, other_context, scalars, part):
    rows, width = queries.shape[1:]
    span = context.shape[1]
    count = width // HEAD_DIM
    step = rows // PARTS
    seen = WINDOW + step
    start = part * step + span - rows - WINDOW
    scale = HEAD_DIM ** (-0.5)

    def kernel(first_ref, q_ref, mine_ref, other_ref, out_ref):
        run = pl.program_id(0)
        mine = mine_ref[0, start : start + seen, :]
        other = other_ref[0, start : start + seen, :]
        k = jnp.where(first_ref[2] == 0, mine, other)
        v = jnp.where(first_ref[2] == 0, other, mine)
        query_pos = lax.broadcasted_iota(jnp.int32, (step, seen), 0)
        key_pos = lax.broadcasted_iota(jnp.int32, (step, seen), 1)
        distance = query_pos + WINDOW - key_pos
        allowed = (distance >= 0) & (distance < WINDOW)
        allowed = allowed & (key_pos >= -first_ref[run] - start)
        for head in range(count):
            cols = slice(head * HEAD_DIM, (head + 1) * HEAD_DIM)
            scores = lax.dot_general(
                q_ref[0, :, cols], k, (((1,), (1,)), ((), ())), preferred_element_type=jnp.float32
            )
            scores = jnp.where(allowed, scores * scale, -1e30)
            raised = jnp.exp(scores - jnp.max(scores, axis=1, keepdims=True))
            total = jnp.sum(raised, axis=1, keepdims=True)
            mixed = jnp.dot(raised.astype(jnp.bfloat16), v, preferred_element_type=jnp.float32)
            out_ref[0, :, cols] = (mixed / total).astype(jnp.bfloat16)

    whole = pl.BlockSpec((1, span, HEAD_DIM), lambda run, first: (run, 0, 0))
    return call(
        kernel,
        (2,),
        1,
        [pl.BlockSpec((1, step, width), lambda run, first: (run, part, 0)), whole, whole],
        pl.BlockSpec((1, step, width), lambda run, first: (run, 0, 0)),
        jax.ShapeDtypeStruct((2, step, width), jnp.bfloat16),
        flops=2 * step * width * seen * 4,
        moved=2 * (2 * queries.size // PARTS + 2 * context.size),
    )(scalars, queries, context, other_context)


def packed(parity, parts):
    arrays = [array for part in parts for array, *_ in part]
    rows = arrays[0].shape[0]
    width = sum(-(-size // 128) * 128 for _, _, size in parts[0])

    def kernel(parity_ref, *refs):
        ins, outs = refs[:-2], refs[-2:]
        for swap in range(2):

            @pl.when(parity_ref[0] == swap)
            def _():
                for h in range(2):
                    out = outs[h ^ swap]
                    at = 0
                    for i, (_, start, size) in enumerate(parts[h]):
                        ref = ins[h * len(parts[0]) + i]
                        out[:, at : at + size] = ref[:, start : start + size]
                        full = -(-size // 128) * 128
                        if full > size:
                            out[:, at + size : at + full] = jnp.zeros(
                                (rows, full - size), jnp.bfloat16
                            )
                        at += full

    def spec(shape):
        return pl.BlockSpec(shape, lambda i, parity: (0, 0))

    return call(
        kernel,
        (1,),
        1,
        [spec(array.shape) for array in arrays],
        [spec((rows, width))] * 2,
        [jax.ShapeDtypeStruct((rows, width), jnp.bfloat16)] * 2,
        moved=8 * rows * width,
    )(parity, *arrays)


def per_device(tokens, attn_gain, w_query, w_key, w_value, w_out, mlp_gain, w_gate, w_up, w_down):
    rows = tokens.shape[0]
    yl, yh, core = (lax.axis_index(name) for name in ("yl", "yh", "c"))
    place = lax.axis_index(PLANE)
    plane = lax.axis_size("x") * lax.axis_size("z")
    me = jnp.reshape(yh * 2 + core, (1,)).astype(jnp.int32)
    parity = jnp.reshape(yl, (1,)).astype(jnp.int32)
    out_t, down_t = w_out.T, w_down.T
    kv_width = w_key.shape[1]
    heads = w_query.shape[1] // 2
    units = w_gate.shape[1] // 2

    attn_rows = column_rows(
        packed(
            parity,
            [
                [
                    (w_query, h * heads, heads),
                    ((w_key, w_value)[h], 0, kv_width),
                    (out_t, h * heads, heads),
                ]
                for h in range(2)
            ],
        )
    )
    split = heads + kv_width
    attn_full = spread(attn_rows, "z")
    attn_full, out_full = attn_full[..., :split], attn_full[..., split:]
    mlp_rows = column_rows(
        packed(
            parity,
            [[(array, h * units, units) for array in (w_gate, w_up, down_t)] for h in range(2)],
        )
    )
    attn_full = lax.all_gather(attn_full, "x", axis=0, tiled=True)
    normed = normed_rows(me, *column_blocks(tokens), attn_gain)
    mlp_rows, attn_full, normed = lax.optimization_barrier((mlp_rows, attn_full, normed))
    mlp_full = lax.all_gather(mlp_rows[None], PLANE, axis=0, tiled=True)
    out_full = spread(out_full, "x")
    out_full = out_full.reshape(-1, *out_full.shape[2:])
    fresh = projected(normed, attn_full, heads, kv_width).reshape(2, rows, kv_width)
    reach = -(-WINDOW // rows)
    context = [fresh]
    for step in range(1, reach + 1):
        came = lax.ppermute(fresh, PLANE, [(i, (i + step) % plane) for i in range(plane)])
        context.insert(0, jnp.where(place < step, came[::-1], came))
    context = jnp.concatenate(context, axis=1)
    other_context = other_core(context)

    queries = projected(normed, attn_full, 0, heads).reshape(2, rows, heads)
    runs = jnp.stack([yl, 1 - yl])
    first_key = ((runs * plane + place - reach) * rows).astype(jnp.int32)
    scalars = jnp.concatenate([first_key, jnp.reshape(core, (1,)).astype(jnp.int32)])
    part = rows // PARTS
    outputs = []
    for i in range(PARTS):
        attended = window_attention(queries, context, other_context, scalars, i)
        attn_share = column_sum(*head_terms(me, attended, out_full))
        residual = tokens[i * part : (i + 1) * part]
        if i > 0:
            residual, stream = lax.optimization_barrier((residual, stream))
        stream = (residual.astype(jnp.float32) + attn_share).astype(jnp.bfloat16)
        blocks = column_blocks(stream)
        terms = unit_terms(me, *blocks, mlp_gain, mlp_full)
        mlp_share = column_sum(*terms)
        outputs.append((stream.astype(jnp.float32) + mlp_share).astype(jnp.bfloat16))
    return jnp.concatenate(outputs, axis=0)


def solution(mesh):
    split = Mesh(mesh.devices.reshape(2, 4, 8, 2, 2), ("yl", "x", "z", "yh", "c"))
    both = P(SEQ, FEATURES)
    down = P(FEATURES, SEQ)
    placed = (both, P(), both, both, both, down, P(), both, both, down)

    return jax.shard_map(per_device, mesh=split, in_specs=placed, out_specs=both, check_vma=False)
```

```python
import jax
import jax.numpy as jnp
from jax import lax
from jax.experimental import pallas as pl
from jax.experimental.pallas import tpu as pltpu
from jax.sharding import Mesh
from jax.sharding import PartitionSpec as P

HEAD_DIM = 128
WINDOW = 1024
SEQ = ("yl", "x", "z")
FEATURES = ("yh", "c")
PLANE = ("x", "z")
PARTS = 2


def spread(value, axis):
    length = lax.axis_size(axis)
    return lax.all_to_all(
        jnp.broadcast_to(value[None], (length, *value.shape)), axis, 0, 0, tiled=True
    )


def other_core(value):
    return lax.ppermute(value, "c", [(0, 1), (1, 0)])


def column_partner(value, flip):
    return lax.ppermute(value, ("yl", "yh"), [(i, i ^ flip) for i in range(4)])


def ordered(flag, first, second):
    return jnp.where(flag == 0, first, second), jnp.where(flag == 0, second, first)


def column_rows(sends):
    received = [
        lax.ppermute(send, ("yl", "c"), [(yl * 2 + c, c * 2 + (yl ^ swap)) for yl in range(2) for c in range(2)])
        for swap, send in enumerate(sends)
    ]
    return jnp.stack(ordered(lax.axis_index("c"), *received))


def column_blocks(share):
    blocks = [share]
    for flip in (1, 2, 3):
        blocks.append(column_partner(share, flip))
    mine = jnp.stack(blocks)
    return mine, other_core(mine)


def call(kernel, grid, scalars, in_specs, out_specs, out_shape, scratch=(), flops=0, moved=0, grant=32):
    return pl.pallas_call(
        kernel,
        grid_spec=pltpu.PrefetchScalarGridSpec(
            num_scalar_prefetch=scalars,
            grid=grid,
            in_specs=in_specs,
            out_specs=out_specs,
            scratch_shapes=scratch,
        ),
        out_shape=out_shape,
        compiler_params=pltpu.CompilerParams(vmem_limit_bytes=grant * 1024 * 1024),
        cost_estimate=pl.CostEstimate(flops=flops, bytes_accessed=moved, transcendentals=0),
    )


def store_normed(me_ref, mine_ref, theirs_ref, gain_ref, out_ref, run, at):
    n, f = mine_ref.shape[1:]
    parts = [
        (half * 2 + other, (mine_ref, theirs_ref)[other][run * 2 + half].astype(jnp.float32))
        for half in range(2)
        for other in range(2)
    ]
    squares = sum(jnp.sum(x * x, axis=1, keepdims=True) for _, x in parts)
    scale = lax.rsqrt(squares / (len(parts) * f) + 1e-06)
    for flip, x in parts:
        column = pl.multiple_of((me_ref[0] ^ flip) * f, f)
        gain = gain_ref[:, pl.ds(column, f)]
        out_ref[pl.ds(at, n), pl.ds(column, f)] = (x * scale * gain).astype(jnp.bfloat16)


def normed_rows(me, mine, theirs, gain):
    rows, f = mine.shape[1:]
    step = min(256, rows)

    def kernel(me_ref, mine_ref, theirs_ref, gain_ref, out_ref):
        store_normed(me_ref, mine_ref, theirs_ref, gain_ref, out_ref, 0, 0)

    block = pl.BlockSpec((2, step, f), lambda run, i, me: (run, i, 0))
    tiles = rows // step
    return call(
        kernel,
        (2, tiles),
        1,
        [block, block, pl.BlockSpec((1, 4 * f), lambda run, i, me: (0, 0))],
        pl.BlockSpec((step, 4 * f), lambda run, i, me: (run * tiles + i, 0)),
        jax.ShapeDtypeStruct((2 * rows, 4 * f), jnp.bfloat16),
        flops=rows * f * 100,
        moved=rows * f * 32,
    )(me, mine, theirs, gain[None])


def unit_terms(me, mine, theirs, gain, weights):
    rows, f = mine.shape[1:]
    chips, runs, r = weights.shape[:3]
    d = chips * runs * r
    width = weights.shape[3] // 3
    step = 256
    steps = width // step

    def kernel(
        me_ref, mine_ref, theirs_ref, gain_ref, gate_ref, up_ref, all_ref, near_ref, away_ref,
        normed, hidden, down_ref, arrived,
    ):
        j = pl.program_id(0)
        fetch = pltpu.make_async_copy(all_ref.at[:, :, :, 2 * width :], down_ref, arrived)

        @pl.when(j == 0)
        def _():
            fetch.start()
            for run in range(2):
                store_normed(
                    me_ref, mine_ref, theirs_ref, gain_ref, normed, run, run * rows
                )

        @pl.when(j < steps)
        def _():
            gate = up = 0.0
            for run in range(runs):
                x = normed[:, run * chips * r : (run + 1) * chips * r]
                gate_rows = gate_ref[:, run].reshape(chips * r, step)
                gate = gate + jnp.dot(x, gate_rows, preferred_element_type=jnp.float32)
                up_rows = up_ref[:, run].reshape(chips * r, step)
                up = up + jnp.dot(x, up_rows, preferred_element_type=jnp.float32)
            hidden[j] = (gate / (1.0 + jnp.exp(-gate)) * up).astype(jnp.bfloat16)

        @pl.when(j == steps)
        def _():
            fetch.wait()

        @pl.when(j >= steps)
        def _():
            left = jnp.concatenate([hidden[i] for i in range(steps)], axis=1)
            for out, flip in ((away_ref, 2 * (j - steps) + 1), (near_ref, 2 * (j - steps))):
                term = lax.dot_general(
                    left,
                    feature_rows(down_ref, me_ref[0] ^ flip),
                    (((1,), (1,)), ((), ())),
                    preferred_element_type=jnp.float32,
                )
                out[...] = term.astype(out.dtype)

    def whole(shape):
        return pl.BlockSpec(shape, lambda j, me: (0,) * len(shape))

    def weight(part):
        return pl.BlockSpec(
            (chips, runs, r, step),
            lambda j, me: (0, 0, 0, part * steps + jnp.minimum(j, steps - 1)),
        )

    shape = (2 * rows, 2 * f)
    return call(
        kernel,
        (steps + 2,),
        1,
        [whole(mine.shape), whole(mine.shape), whole((1, 4 * f))]
        + [weight(0), weight(1), pl.BlockSpec(memory_space=pl.ANY)],
        [pl.BlockSpec((2 * rows, f), lambda j, me: (0, jnp.maximum(j - steps, 0)))] * 2,
        [jax.ShapeDtypeStruct(shape, jnp.float32), jax.ShapeDtypeStruct(shape, jnp.bfloat16)],
        [
            pltpu.VMEM((2 * rows, 4 * f), jnp.bfloat16),
            pltpu.VMEM((steps, 2 * rows, step), jnp.bfloat16),
            pltpu.VMEM((chips, runs, r, width), jnp.bfloat16),
            pltpu.SemaphoreType.DMA,
        ],
        flops=2 * 2 * rows * width * (2 * d + 4 * f),
        moved=2 * weights.size + 16 * rows * f * 2,
    )(me, mine, theirs, gain[None], weights, weights, weights)


def projected(left, weights, start, width):
    n, d = left.shape
    chips, runs, r = weights.shape[:3]
    step = 256

    def kernel(x_ref, w_ref, out_ref):
        total = 0.0
        for run in range(runs):
            w = w_ref[:, run].reshape(chips * r, width)
            x = x_ref[:, run * chips * r : (run + 1) * chips * r]
            total = total + jnp.dot(x, w, preferred_element_type=jnp.float32)
        out_ref[...] = total.astype(jnp.bfloat16)

    return call(
        kernel,
        (n // step,),
        0,
        [
            pl.BlockSpec((step, d), lambda i: (i, 0)),
            pl.BlockSpec((chips, runs, r, width), lambda i: (0, 0, 0, start // width)),
        ],
        pl.BlockSpec((step, width), lambda i: (i, 0)),
        jax.ShapeDtypeStruct((n, width), jnp.bfloat16),
        flops=2 * n * d * width,
        moved=2 * (n * d + d * width + n * width),
        grant=58,
    )(left, weights)


def feature_rows(weights_ref, block):
    chips, _, r, k = weights_ref.shape
    half = chips // 2
    at = pl.multiple_of(lax.rem(block, 2) * half, half)
    return weights_ref[pl.ds(at, half), lax.div(block, 2)].reshape(half * r, k)


def head_terms(me, attended, weights):
    rows, width = attended.shape[1:]
    f = weights.shape[0] * weights.shape[1] * weights.shape[2] // 4

    def kernel(me_ref, left_ref, weights_ref, near_ref, away_ref):
        left = left_ref[...].reshape(2 * rows, width)
        at = 2 * pl.program_id(0)
        for out, flip in ((away_ref, at + 1), (near_ref, at)):
            term = lax.dot_general(
                left,
                feature_rows(weights_ref, me_ref[0] ^ flip),
                (((1,), (1,)), ((), ())),
                preferred_element_type=jnp.float32,
            )
            out[...] = term.astype(out.dtype)

    shape = (2 * rows, 2 * f)
    return call(
        kernel,
        (2,),
        1,
        [
            pl.BlockSpec((2, rows, width), lambda i, me: (0, 0, 0)),
            pl.BlockSpec((*weights.shape[:3], width), lambda i, me: (0, 0, 0, 0)),
        ],
        [pl.BlockSpec((2 * rows, f), lambda i, me: (0, i))] * 2,
        [jax.ShapeDtypeStruct(shape, jnp.float32), jax.ShapeDtypeStruct(shape, jnp.bfloat16)],
        flops=4 * rows * 4 * f * width,
        moved=8 * f * width + 24 * rows * f,
    )(me, attended, weights)


def column_sum(near, away):
    rows, f = near.shape[0] // 2, near.shape[1] // 2
    both = near + other_core(away).astype(jnp.float32)
    total = both[:rows, :f]
    sent = (
        (both[:rows, f:], 1),
        (both[rows:, :f], 2),
        (both[rows:, f:], 3),
    )
    for value, flip in sent:
        came = column_partner(value.astype(jnp.bfloat16), flip)
        total = total + came.astype(jnp.float32)
    return total


def window_attention(queries, context, other_context, scalars, part):
    rows, width = queries.shape[1:]
    span = context.shape[1]
    count = width // HEAD_DIM
    step = rows // PARTS
    seen = WINDOW + step
    start = part * step + span - rows - WINDOW
    scale = HEAD_DIM ** (-0.5)

    def kernel(first_ref, q_ref, mine_ref, other_ref, out_ref):
        run = pl.program_id(0)
        mine = mine_ref[0, start : start + seen, :]
        other = other_ref[0, start : start + seen, :]
        k = jnp.where(first_ref[2] == 0, mine, other)
        v = jnp.where(first_ref[2] == 0, other, mine)
        query_pos = lax.broadcasted_iota(jnp.int32, (step, seen), 0)
        key_pos = lax.broadcasted_iota(jnp.int32, (step, seen), 1)
        distance = query_pos + WINDOW - key_pos
        allowed = (distance >= 0) & (distance < WINDOW)
        allowed = allowed & (key_pos >= -first_ref[run] - start)
        for head in range(count):
            cols = slice(head * HEAD_DIM, (head + 1) * HEAD_DIM)
            scores = lax.dot_general(
                q_ref[0, :, cols], k, (((1,), (1,)), ((), ())), preferred_element_type=jnp.float32
            )
            scores = jnp.where(allowed, scores * scale, -1e30)
            raised = jnp.exp(scores - jnp.max(scores, axis=1, keepdims=True))
            total = jnp.sum(raised, axis=1, keepdims=True)
            mixed = jnp.dot(raised.astype(jnp.bfloat16), v, preferred_element_type=jnp.float32)
            out_ref[0, :, cols] = (mixed / total).astype(jnp.bfloat16)

    whole = pl.BlockSpec((1, span, HEAD_DIM), lambda run, first: (run, 0, 0))
    return call(
        kernel,
        (2,),
        1,
        [pl.BlockSpec((1, step, width), lambda run, first: (run, part, 0)), whole, whole],
        pl.BlockSpec((1, step, width), lambda run, first: (run, 0, 0)),
        jax.ShapeDtypeStruct((2, step, width), jnp.bfloat16),
        flops=2 * step * width * seen * 4,
        moved=2 * (2 * queries.size // PARTS + 2 * context.size),
    )(scalars, queries, context, other_context)


def packed(parity, parts):
    arrays = [array for part in parts for array, *_ in part]
    rows = arrays[0].shape[0]
    width = sum(-(-size // 128) * 128 for _, _, size in parts[0])

    def kernel(parity_ref, *refs):
        ins, outs = refs[:-2], refs[-2:]
        for swap in range(2):

            @pl.when(parity_ref[0] == swap)
            def _():
                for h in range(2):
                    out = outs[h ^ swap]
                    at = 0
                    for i, (_, start, size) in enumerate(parts[h]):
                        ref = ins[h * len(parts[0]) + i]
                        out[:, at : at + size] = ref[:, start : start + size]
                        full = -(-size // 128) * 128
                        if full > size:
                            out[:, at + size : at + full] = jnp.zeros(
                                (rows, full - size), jnp.bfloat16
                            )
                        at += full

    def spec(shape):
        return pl.BlockSpec(shape, lambda i, parity: (0, 0))

    return call(
        kernel,
        (1,),
        1,
        [spec(array.shape) for array in arrays],
        [spec((rows, width))] * 2,
        [jax.ShapeDtypeStruct((rows, width), jnp.bfloat16)] * 2,
        moved=8 * rows * width,
    )(parity, *arrays)


def per_device(tokens, attn_gain, w_query, w_key, w_value, w_out, mlp_gain, w_gate, w_up, w_down):
    rows = tokens.shape[0]
    yl, yh, core = (lax.axis_index(name) for name in ("yl", "yh", "c"))
    place = lax.axis_index(PLANE)
    plane = lax.axis_size("x") * lax.axis_size("z")
    me = jnp.reshape(yh * 2 + core, (1,)).astype(jnp.int32)
    parity = jnp.reshape(yl, (1,)).astype(jnp.int32)
    out_t, down_t = w_out.T, w_down.T
    kv_width = w_key.shape[1]
    heads = w_query.shape[1] // 2
    units = w_gate.shape[1] // 2

    attn_rows = column_rows(
        packed(
            parity,
            [
                [
                    (w_query, h * heads, heads),
                    ((w_key, w_value)[h], 0, kv_width),
                    (out_t, h * heads, heads),
                ]
                for h in range(2)
            ],
        )
    )
    split = heads + kv_width
    attn_full = spread(attn_rows, "z")
    attn_full, out_full = attn_full[..., :split], attn_full[..., split:]
    mlp_rows = column_rows(
        packed(
            parity,
            [[(array, h * units, units) for array in (w_gate, w_up, down_t)] for h in range(2)],
        )
    )
    attn_full = lax.all_gather(attn_full, "x", axis=0, tiled=True)
    normed = normed_rows(me, *column_blocks(tokens), attn_gain)
    mlp_rows, attn_full, normed = lax.optimization_barrier((mlp_rows, attn_full, normed))
    mlp_full = lax.all_gather(mlp_rows[None], PLANE, axis=0, tiled=True)
    out_full = spread(out_full, "x")
    out_full = out_full.reshape(-1, *out_full.shape[2:])
    fresh = projected(normed, attn_full, heads, kv_width).reshape(2, rows, kv_width)
    reach = -(-WINDOW // rows)
    context = [fresh]
    for step in range(1, reach + 1):
        came = lax.ppermute(fresh, PLANE, [(i, (i + step) % plane) for i in range(plane)])
        context.insert(0, jnp.where(place < step, came[::-1], came))
    context = jnp.concatenate(context, axis=1)
    other_context = other_core(context)

    queries = projected(normed, attn_full, 0, heads).reshape(2, rows, heads)
    runs = jnp.stack([yl, 1 - yl])
    first_key = ((runs * plane + place - reach) * rows).astype(jnp.int32)
    scalars = jnp.concatenate([first_key, jnp.reshape(core, (1,)).astype(jnp.int32)])
    part = rows // PARTS
    outputs = []
    for i in range(PARTS):
        attended = window_attention(queries, context, other_context, scalars, i)
        attn_share = column_sum(*head_terms(me, attended, out_full))
        residual = tokens[i * part : (i + 1) * part]
        if i > 0:
            residual, stream = lax.optimization_barrier((residual, stream))
        stream = (residual.astype(jnp.float32) + attn_share).astype(jnp.bfloat16)
        blocks = column_blocks(stream)
        terms = unit_terms(me, *blocks, mlp_gain, mlp_full)
        mlp_share = column_sum(*terms)
        outputs.append((stream.astype(jnp.float32) + mlp_share).astype(jnp.bfloat16))
    return jnp.concatenate(outputs, axis=0)


def solution(mesh):
    split = Mesh(mesh.devices.reshape(2, 4, 8, 2, 2), ("yl", "x", "z", "yh", "c"))
    both = P(SEQ, FEATURES)
    down = P(FEATURES, SEQ)
    placed = (both, P(), both, both, both, down, P(), both, both, down)

    return jax.shard_map(per_device, mesh=split, in_specs=placed, out_specs=both, check_vma=False)
```
